256 devices in a mesh: dp: 32 (over y, z), mp: 8 (over x, core).
Axes of the slice: x: 4, y: 4, z: 8, core: 2. Of those that a mesh axis runs over, the one named last changes fastest.
Arguments:
- tokens: bfloat16 [32, 1024, 1280], P('dp', 'mp'), may hold values from -6 to 6
- sizes: float32 [32, 1024], P('dp'), may hold values from 1 to 8
- ln1_gain: float32 [1280], replicated, may hold values from 0.25 to 1.75
- qkv_weight: bfloat16 [3, 1280, 1280], P(None, 'dp', 'mp'), may hold values from -0.15625 to 0.15625
- proj_weight: bfloat16 [1280, 1280], P('mp', 'dp'), may hold values from -0.15625 to 0.15625
- ln2_gain: float32 [1280], replicated, may hold values from 0.25 to 1.75
- fc1_weight: bfloat16 [1280, 5120], P('dp', 'mp'), may hold values from -0.15625 to 0.15625
- fc1_bias: float32 [5120], P('mp'), may hold values from -3 to 3
- fc2_weight: bfloat16 [5120, 1280], P('mp', 'dp'), may hold values from -0.078125 to 0.078125
- pair_source: int32 [32, 16], P('dp'), may hold values from 0 to 1022, as said below
- pair_target: int32 [32, 16], P('dp'), may hold values from 1 to 1023, as said below
- kept_order: int32 [32, 1008], P('dp'), may hold values from 0 to 1023, as said below
Outputs:
- merged_out: bfloat16 [32, 1008, 1280], P('dp', 'mp')
The draws below stay inside these ranges and needn't reach their ends.
Inputs may be any that keep to these rules, and one draw needn't show every extreme that they name: `pair_source`: in each image the 16 entries are distinct even token indices. `pair_target`: odd token indices; several sources may join the same target. `kept_order`: in each image every token index that is not in pair_source appears exactly once.
All inputs are finite; a program needn't handle non-finite values.
Results may differ from the reference program's by a relative error of at most 0.017.
Values may be sent and summed in bfloat16 or wider, within the bound.
No kernel may reach another device: no remote copies, remote signals or barrier semaphores. Data moves between devices by JAX's collectives and lax.ppermute only.
A program may use at most 64 MiB of HBM per device.

```python
import math
import jax
import jax.numpy as jnp
from jax import lax

D = 1280
HEADS = 16
FF = 5120
N = 1024
R = 16
IMAGES = 32


def merge_plan(key):
    image_keys = jax.random.split(jax.random.fold_in(key, 7), IMAGES)

    def one_plan(image_key):
        first, second, third = jax.random.split(image_key, 3)
        shuffled = jax.random.permutation(first, N // 2).astype(jnp.int32)
        sources = 2 * shuffled[:R]
        targets = 2 * jax.random.randint(second, (R,), 0, N // 2).astype(jnp.int32) + 1
        kept_even = 2 * shuffled[R:]
        odd_tokens = 2 * jnp.arange(N // 2, dtype=jnp.int32) + 1
        remaining = jnp.concatenate([kept_even, odd_tokens])
        ordered = jax.random.permutation(third, remaining).astype(jnp.int32)
        return (sources, targets, ordered)
    return jax.vmap(one_plan)(image_keys)


def draw_pair_source(key, part):
    return merge_plan(key)[0]


def draw_pair_target(key, part):
    return merge_plan(key)[1]


def draw_kept_order(key, part):
    return merge_plan(key)[2]


def shard_levels(own_key, shape, cuts, low, high):
    def one(dim, blocks):
        heights = jax.random.uniform(jax.random.fold_in(jax.random.fold_in(own_key, 6), dim), (blocks,), jnp.float32, low / len(cuts), high / len(cuts))
        return jnp.repeat(jnp.exp(heights), shape[dim] // blocks).reshape((-1,) + (1,) * (len(shape) - dim - 1))

    factor_of = one(*cuts[0])
    for cut in cuts[1:]:
        factor_of = factor_of * one(*cut)
    return factor_of


def centred(key, extent, deviation, most, cuts=(), kind=jnp.bfloat16):
    values = deviation * jax.random.normal(key, extent, jnp.float32)
    if cuts:
        values = values * shard_levels(key, extent, cuts, -0.22, 0.18)
    return jnp.clip(values, -most, most).astype(kind)


def setup_inputs(seed: int = 0) -> dict:
    streams_of = jax.random.split(jax.random.key(seed), 13)
    return {
        "tokens": centred(streams_of[0], (IMAGES, N, D), 1.0, 6.0, ((0, 32), (1, 8))),
        "sizes": jnp.clip(jnp.exp(math.log(8.0) - 2.0794415 * jax.random.uniform(streams_of[1], (IMAGES, N), jnp.float32) ** shard_levels(streams_of[1], (IMAGES, N), ((0, 32),), -0.2, 0.2)), 1.0, 8.0),
        "ln1_gain": jnp.clip(1.0 + 0.15 * jax.random.normal(streams_of[2], (D,), jnp.float32), 0.25, 1.75),
        "qkv_weight": centred(streams_of[3], (3, D, D), D ** -0.5, 0.15625, ((1, 32), (2, 8))),
        "proj_weight": centred(streams_of[4], (D, D), D ** -0.5, 0.15625, ((0, 8), (1, 32))),
        "ln2_gain": jnp.clip(1.0 + 0.15 * jax.random.normal(streams_of[5], (D,), jnp.float32), 0.25, 1.75),
        "fc1_weight": centred(streams_of[6], (D, FF), D ** -0.5, 0.15625, ((0, 32), (1, 8))),
        "fc1_bias": centred(streams_of[7], (FF,), 0.5, 3.0, ((0, 8),), jnp.float32),
        "fc2_weight": centred(streams_of[8], (FF, D), FF ** -0.5, 0.078125, ((0, 8), (1, 32))),
        "pair_source": draw_pair_source(jax.random.fold_in(streams_of[12], 71), 0),
        "pair_target": draw_pair_target(jax.random.fold_in(streams_of[12], 71), 0),
        "kept_order": draw_kept_order(jax.random.fold_in(streams_of[12], 71), 0),
    }


def layer_norm(values, gain):
    center = values - lax.optimization_barrier(jnp.mean(values, axis=-1, keepdims=True))
    spread = lax.optimization_barrier(jnp.mean(center * center, axis=-1, keepdims=True))
    return center * lax.rsqrt(spread + 1e-06) * gain

def one_image(tokens, sizes, source_ids, target_ids, order, ln1_gain, qkv_weight, proj_weight, ln2_gain, fc1_weight, fc1_bias, fc2_weight):
    width = tokens.shape[1]
    head_size = width // HEADS
    base = tokens.astype(jnp.float32)
    normed = layer_norm(base, ln1_gain).astype(jnp.bfloat16)
    query = jnp.dot(normed, qkv_weight[0], preferred_element_type=jnp.float32).astype(jnp.bfloat16)
    keys = jnp.dot(normed, qkv_weight[1], preferred_element_type=jnp.float32).astype(jnp.bfloat16)
    values = jnp.dot(normed, qkv_weight[2], preferred_element_type=jnp.float32).astype(jnp.bfloat16)
    length = tokens.shape[0]
    query = query.reshape(length, HEADS, head_size).astype(jnp.float32)
    keys = keys.reshape(length, HEADS, head_size).astype(jnp.float32)
    values = values.reshape(length, HEADS, head_size).astype(jnp.float32)
    scores = jnp.einsum('qhe,khe->hqk', query, keys) / math.sqrt(head_size) + jnp.log(sizes)[None, None, :]
    weights = jax.nn.softmax(scores, axis=-1).astype(jnp.bfloat16)
    attended = jnp.einsum('hqk,khe->qhe', weights.astype(jnp.float32), values).astype(jnp.bfloat16)
    attended = attended.reshape(length, width)
    residual = base + jnp.dot(attended, proj_weight, preferred_element_type=jnp.float32)
    positions = jnp.arange(length, dtype=jnp.int32)
    hits = (positions[None, :] == source_ids[:, None]).astype(jnp.int32)
    destination = positions + lax.optimization_barrier(jnp.sum(hits * (target_ids[:, None] - positions[None, :]), axis=0))
    table = (order[:, None] == destination[None, :]).astype(jnp.float32)
    numerator = jnp.dot(table, sizes[:, None] * residual, precision=lax.Precision.HIGHEST)
    merged_size = jnp.dot(table, sizes, precision=lax.Precision.HIGHEST)
    merged = numerator / merged_size[:, None]
    normed_two = layer_norm(merged, ln2_gain).astype(jnp.bfloat16)
    hidden = jax.nn.gelu(jnp.dot(normed_two, fc1_weight, preferred_element_type=jnp.float32) + fc1_bias).astype(jnp.bfloat16)
    return (merged + jnp.dot(hidden, fc2_weight, preferred_element_type=jnp.float32)).astype(jnp.bfloat16)

def reference(tokens, sizes, ln1_gain, qkv_weight, proj_weight, ln2_gain, fc1_weight, fc1_bias, fc2_weight, pair_source, pair_target, kept_order):

    def apply(item):
        return one_image(item[0], item[1], item[2], item[3], item[4], ln1_gain, qkv_weight, proj_weight, ln2_gain, fc1_weight, fc1_bias, fc2_weight)
    return lax.map(apply, (tokens, sizes, pair_source, pair_target, kept_order))
```

```python
import functools
import math

import jax
import jax.numpy as jnp
from jax import lax
from jax.experimental import pallas as pl
from jax.experimental.pallas import tpu as pltpu
from jax.sharding import Mesh, PartitionSpec as P

HEADS = 16
BF = jnp.bfloat16
F32 = jnp.float32
VMEM = pltpu.VMEM
SMEM = pltpu.SMEM


def shift(x, axis, by):
    n = lax.axis_size(axis)
    return lax.ppermute(x, axis, [(i, (i + by) % n) for i in range(n)])


def layer_norm(values, gain):
    center = values - jnp.mean(values, axis=-1, keepdims=True)
    spread = jnp.mean(center * center, axis=-1, keepdims=True)
    return center * lax.rsqrt(spread + 1e-06) * gain


def dot_t(a, b):
    return lax.dot_general(a, b, (((1,), (1,)), ((), ())), preferred_element_type=F32)


def dot(a, b):
    return jnp.dot(a, b, preferred_element_type=F32)


def whole(n, space=VMEM):
    return [pl.BlockSpec(memory_space=space)] * n


def attention_kernel(hs, y_ref, xn_ref, w0, w1, w2, w3, kx_ref, keep_ref, send_ref,
                     out_keep, out_send, w_scr, qkv_scr, q_scr, k_scr, v_scr, att_scr):
    tokens = xn_ref.shape[0]
    rows = w0.shape[0]
    y = y_ref[0]
    for j, block in enumerate((w0, w1, w2, w3)):
        start = pl.multiple_of(lax.rem(y + j, 4) * rows, 64)
        w_scr[pl.ds(start, rows), :] = block[...]
    chunk = 256
    for r in range(0, tokens, chunk):
        qkv_scr[r : r + chunk, :] = dot(xn_ref[r : r + chunk, :], w_scr[...])
    scale = math.log2(math.e) / math.sqrt(hs)

    def piece(j):
        first, offset = divmod(hs * j, 128)
        width = 128 if offset + hs <= 128 else 256
        x = qkv_scr[:, 128 * first : 128 * first + width]
        if offset:
            x = pltpu.roll(x, width - offset, 1)
        return x[:, :128]

    lane = lax.broadcasted_iota(jnp.int32, (tokens, 128), 1)
    real = lane < hs
    for h in range(2):
        ones = jnp.where(lane < hs + 3, 1.0, 0.0)
        q_scr[...] = jnp.where(real, piece(h), ones).astype(BF)
        k_scr[...] = jnp.where(real, piece(2 + h), kx_ref[...]).astype(BF)
        v_scr[...] = jnp.where(real, piece(4 + h), ones).astype(BF)
        for r in range(0, tokens, chunk):
            s = dot_t(q_scr[r : r + chunk, :], k_scr[...])
            top = jnp.max(s, axis=-1, keepdims=True)
            p = jnp.exp2((s - top) * scale).astype(BF)
            o = dot(p, v_scr[...])
            o = o / o[:, hs : hs + 1]
            o = jnp.where(lane[:chunk] < hs, o, 0.0)
            att_scr[r : r + chunk, 128 * h : 128 * h + 128] = o.astype(BF)
    out_send[...] = dot(send_ref[...], att_scr[...]).astype(BF)
    out_keep[...] = dot(keep_ref[...], att_scr[...]).astype(BF)


def attention(y, xn, blocks, kx, keep, send, hs):
    tokens = xn.shape[0]
    cols = blocks[0].shape[1]
    rows = keep.shape[0]
    return pl.pallas_call(
        functools.partial(attention_kernel, hs),
        out_shape=[jax.ShapeDtypeStruct((rows, 256), BF)] * 2,
        in_specs=whole(1, SMEM) + whole(8),
        out_specs=whole(2),
        scratch_shapes=[
            pltpu.VMEM((4 * blocks[0].shape[0], cols), BF),
            pltpu.VMEM((tokens, cols), F32),
            pltpu.VMEM((tokens, 128), BF),
            pltpu.VMEM((tokens, 128), BF),
            pltpu.VMEM((tokens, 128), BF),
            pltpu.VMEM((tokens, 256), BF),
        ],
        compiler_params=pltpu.CompilerParams(vmem_limit_bytes=48 * 2**20),
        cost_estimate=pl.CostEstimate(flops=5_000_000_000, bytes_accessed=8_000_000, transcendentals=2_000_000),
        name="attention",
    )(y, xn, *blocks, kx, keep, send)


def mlp_weights_kernel(yz_ref, *refs):
    *blocks, up, down = refs
    half = up.shape[2]
    zs = len(blocks)
    y, z = yz_ref[0], yz_ref[1]
    ys = blocks[0].shape[0]
    for k, block in enumerate(blocks):
        for j in range(ys):
            at = lax.rem(y + j, ys) * zs + lax.rem(z + k, zs)
            up[at] = block[j, :, :half]
            down[at] = block[j, :, half:]


def mlp_weights(yz, blocks):
    ys, rows, cols = blocks[0].shape
    total = ys * len(blocks)
    return pl.pallas_call(
        mlp_weights_kernel,
        out_shape=[jax.ShapeDtypeStruct((total, rows, cols // 2), BF)] * 2,
        in_specs=whole(1, SMEM) + whole(len(blocks)),
        out_specs=whole(2),
        compiler_params=pltpu.CompilerParams(vmem_limit_bytes=16 * 2**20),
        cost_estimate=pl.CostEstimate(flops=1_000_000, bytes_accessed=6_000_000, transcendentals=0),
        name="mlp_weights",
    )(yz, *blocks)


def turned(table, x, c):
    blocks = table.reshape(4, 2, 128)
    blocks = lax.dynamic_slice_in_dim(jnp.concatenate([blocks, blocks]), x, 4, 0)
    mine = lax.dynamic_index_in_dim(blocks, c, 1, keepdims=False)
    other = lax.dynamic_index_in_dim(blocks, 1 - c, 1, keepdims=False)
    return jnp.concatenate([mine.reshape(-1), other.reshape(-1)])


def shards(tokens, sizes, ln1_gain, qkv_weight, proj_weight, ln2_gain, fc1_weight,
           fc1_bias, fc2_weight, pair_source, pair_target, kept_order):
    y, z, x, c = (lax.axis_index(a) for a in ("y", "z", "x", "c"))
    zs = lax.axis_size("z")
    width = tokens.shape[2]
    hs = width // HEADS
    own = tokens[0]
    kept = kept_order.shape[1] // 8

    near = [own] + [shift(own, "x", -k) for k in (1, 2, 3)]
    half = jnp.concatenate(near)
    raw = jnp.concatenate([half, shift(half, "c", 1)])
    normed = layer_norm(raw.astype(F32), ln1_gain).astype(BF)

    qkvp = jnp.concatenate([qkv_weight[0], qkv_weight[1], qkv_weight[2], proj_weight.T], axis=1)
    by_z = lax.all_to_all(jnp.broadcast_to(qkvp, (zs, *qkvp.shape)), "z", 0, 0, tiled=True)
    by_z = by_z.reshape(-1, qkvp.shape[1])
    by_y = [by_z] + [shift(by_z, "y", -j) for j in (1, 2, 3)]

    updown = jnp.concatenate([fc1_weight, fc2_weight.T], axis=1)
    stack = jnp.stack([updown] + [shift(updown, "y", -j) for j in (1, 2, 3)])
    ring = {0: stack}
    for k in range(1, 4):
        ring[k] = shift(ring[k - 1], "z", -1)
        ring[zs - k] = shift(ring[(zs - k + 1) % zs], "z", 1)
    ring[4] = jnp.concatenate([shift(ring[3][:2], "z", -1), shift(ring[5][2:], "z", 1)])
    up, down = mlp_weights(jnp.stack([y, z]), [ring[k] for k in range(zs)])
    up = up.reshape(width, -1)
    down = down.reshape(width, -1)
    ups = (up, shift(up, "c", 1))
    downs = (down, shift(down, "c", 1))
    biases = (fc1_bias, shift(fc1_bias, "c", 1))

    positions = jnp.arange(1024, dtype=jnp.int32)
    hits = positions[None, :] == pair_source[0][:, None]
    dest = positions + jnp.sum(jnp.where(hits, pair_target[0][:, None] - positions[None, :], 0), axis=0)
    dest = turned(dest, x, c)
    size = turned(sizes[0], x, c)
    order = kept_order[0].reshape(4, 2, kept)
    order = jnp.pad(order, ((0, 0), (0, 0), (0, 128 - kept)), constant_values=-1)
    order = turned(order.reshape(-1), x, c).reshape(2, 512)
    table = jnp.where(order[:, :, None] == dest, size, 0.0)
    merged_size = jnp.sum(table, axis=-1, keepdims=True)
    table = (table / jnp.where(merged_size == 0.0, 1.0, merged_size)).astype(BF)
    keep, send = table[0], table[1]
    base = dot(keep[:128], raw)

    bias = jnp.log(size) * math.sqrt(hs)
    high = lax.reduce_precision(bias, 8, 7)
    mid = lax.reduce_precision(bias - high, 8, 7)
    low = bias - high - mid
    lane = jnp.arange(128)[None, :] - hs
    kx = jnp.where(lane == 0, high[:, None], jnp.where(lane == 1, mid[:, None], jnp.where(lane == 2, low[:, None], 0.0)))

    kept_rows, sent_rows = attention(y[None], normed, by_y, kx, keep, send, hs)
    other_rows = shift(sent_rows, "c", 1)

    proj = jnp.concatenate([b[:, 480:] for b in by_y])
    proj = proj.reshape(4, width // 4, 2, hs)
    proj = lax.dynamic_slice_in_dim(jnp.concatenate([proj, proj]), lax.rem(4 - y, 4), 4, 0)
    proj = jnp.pad(proj, ((0, 0), (0, 0), (0, 0), (0, 128 - hs))).reshape(width, 256)
    other_proj = shift(proj, "c", 1)
    partial = dot_t(kept_rows, proj) + dot_t(other_rows, other_proj)
    part = partial.reshape(4, 128, width)
    sent = part.astype(BF)
    merged = base + part[0] + sum(shift(sent[k], "x", k).astype(F32) for k in (1, 2, 3))
    normed2 = layer_norm(merged, ln2_gain).astype(BF)
    rows = jnp.concatenate([normed2] + [shift(normed2, "x", -k) for k in (1, 2, 3)])

    total = 0.0
    for wu, wd, b in zip(ups, downs, biases):
        hidden = jax.nn.gelu(dot(rows, wu) + b).astype(BF)
        total = total + dot_t(hidden, wd)
    part = total.reshape(4, 128, width)
    sent = part.astype(BF)
    out = merged + part[0] + sum(shift(sent[k], "x", k).astype(F32) for k in (1, 2, 3))
    return out[:kept].astype(BF)[None]


def solution(mesh):
    fine = Mesh(mesh.devices.reshape(4, 8, 4, 2), ("y", "z", "x", "c"))
    dp, mp = ("y", "z"), ("x", "c")
    return jax.shard_map(
        shards,
        mesh=fine,
        in_specs=(
            P(dp, mp, None),
            P(dp, None),
            P(),
            P(None, dp, mp),
            P(mp, dp),
            P(),
            P(dp, mp),
            P(mp),
            P(mp, dp),
            P(dp, None),
            P(dp, None),
            P(dp, None),
        ),
        out_specs=P(dp, mp, None),
        check_vma=False,
    )
```

```python
import functools
import math

import jax
import jax.numpy as jnp
from jax import lax
from jax.experimental import pallas as pl
from jax.experimental.pallas import tpu as pltpu
from jax.sharding import Mesh, PartitionSpec as P

HEADS = 16
BF = jnp.bfloat16
F32 = jnp.float32
VMEM = pltpu.VMEM
SMEM = pltpu.SMEM


def shift(x, axis, by):
    n = lax.axis_size(axis)
    return lax.ppermute(x, axis, [(i, (i + by) % n) for i in range(n)])


def layer_norm(values, gain):
    center = values - jnp.mean(values, axis=-1, keepdims=True)
    spread = jnp.mean(center * center, axis=-1, keepdims=True)
    return center * lax.rsqrt(spread + 1e-06) * gain


def dot_t(a, b):
    return lax.dot_general(a, b, (((1,), (1,)), ((), ())), preferred_element_type=F32)


def dot(a, b):
    return jnp.dot(a, b, preferred_element_type=F32)


def whole(n, space=VMEM):
    return [pl.BlockSpec(memory_space=space)] * n


def params(mib):
    return pltpu.CompilerParams(vmem_limit_bytes=mib * 2**20)


def cost(flops, nbytes):
    return pl.CostEstimate(flops=int(flops), bytes_accessed=int(nbytes), transcendentals=0)


def norm_kernel(gain_ref, *refs):
    blocks, outs = refs[:-2], refs[-2:]
    raw_ref, out_ref = outs
    step = 64
    at = 0
    for block in blocks:
        for r in range(0, block.shape[0], step):
            x = block[r : r + step, :]
            raw_ref[at : at + step, :] = x
            out_ref[at : at + step, :] = layer_norm(x.astype(F32), gain_ref[...]).astype(BF)
            at += step


def norm_other_kernel(gain_ref, block, out_ref):
    step = 64

    @pl.loop(0, block.shape[0] // step)
    def _(i):
        at = pl.ds(pl.multiple_of(i * step, step), step)
        out_ref[at, :] = layer_norm(block[at, :].astype(F32), gain_ref[...]).astype(BF)


def norms(gain, blocks):
    rows = sum(b.shape[0] for b in blocks)
    shape = jax.ShapeDtypeStruct((rows, blocks[0].shape[1]), BF)
    return pl.pallas_call(
        norm_kernel,
        out_shape=[shape, shape],
        in_specs=whole(1 + len(blocks)),
        out_specs=whole(2),
        compiler_params=params(16),
        cost_estimate=cost(2e9, 4e6),
        name="norm_mine",
    )(gain, *blocks)


def norm_other(gain, block):
    return pl.pallas_call(
        norm_other_kernel,
        out_shape=jax.ShapeDtypeStruct(block.shape, BF),
        in_specs=whole(2),
        out_specs=whole(1)[0],
        compiler_params=params(16),
        cost_estimate=cost(2e9, 3e6),
        name="norm_other",
    )(gain, block)


def place(blocks, scratch, sems, first, left=0):
    rows = blocks[0].shape[0]
    right = left + scratch.shape[1]
    copies = []
    for j, block in enumerate(blocks):
        start = pl.multiple_of(lax.rem(first + j, len(blocks)) * rows, 64)
        copies.append(pltpu.make_async_copy(block.at[:, left:right], scratch.at[pl.ds(start, rows), :], sems.at[j]))
    for copy in copies:
        copy.start()
    return copies


def attention_kernel(hs, y_ref, xa_ref, xb_ref, w0, w1, w2, w3, kx_ref, keep_ref, send_ref,
                     out_keep, out_send, w_scr, qkv_scr, q_scr, k_scr, v_scr, att_scr, sems):
    half = xa_ref.shape[0]
    tokens = 2 * half
    for copy in place((w0, w1, w2, w3), w_scr, sems, y_ref[0]):
        copy.wait()
    chunk = 256
    qkv_scr[:half, :] = dot(xa_ref[...], w_scr[...])
    qkv_scr[half:, :] = dot(xb_ref[...], w_scr[...])
    scale = math.log2(math.e) / math.sqrt(hs)

    def piece(j):
        first, offset = divmod(hs * j, 128)
        width = 128 if offset + hs <= 128 else 256
        x = qkv_scr[:, 128 * first : 128 * first + width]
        if offset:
            x = pltpu.roll(x, width - offset, 1)
        return x[:, :128]

    lane = lax.broadcasted_iota(jnp.int32, (tokens, 128), 1)
    real = lane < hs
    for h in range(2):
        ones = jnp.where(lane < hs + 3, 1.0, 0.0)
        q_scr[h] = jnp.where(real, piece(h), ones).astype(BF)
        k_scr[h] = jnp.where(real, piece(2 + h), kx_ref[...]).astype(BF)
        v_scr[h] = jnp.where(real, piece(4 + h), ones).astype(BF)
    for h in range(2):
        for r in range(0, tokens, chunk):
            s = dot_t(q_scr[h, r : r + chunk, :], k_scr[h])
            top = jnp.max(s, axis=-1, keepdims=True)
            p = jnp.exp2((s - top) * scale).astype(BF)
            o = dot(p, v_scr[h])
            o = o / o[:, hs : hs + 1]
            o = jnp.where(lane[:chunk] < hs, o, 0.0)
            att_scr[r : r + chunk, 128 * h : 128 * h + 128] = o.astype(BF)
    out_send[...] = dot(send_ref[...], att_scr[...]).astype(BF)
    out_keep[...] = dot(keep_ref[...], att_scr[...]).astype(BF)


def attention(y, xa, xb, blocks, kx, keep, send, hs):
    tokens = 2 * xa.shape[0]
    rows = keep.shape[0]
    return pl.pallas_call(
        functools.partial(attention_kernel, hs),
        out_shape=[jax.ShapeDtypeStruct((rows, 256), BF)] * 2,
        in_specs=whole(1, SMEM) + whole(2) + whole(4, pl.ANY) + whole(3),
        out_specs=whole(2),
        scratch_shapes=[
            pltpu.VMEM((4 * blocks[0].shape[0], 512), BF),
            pltpu.VMEM((tokens, 512), F32),
            pltpu.VMEM((2, tokens, 128), BF),
            pltpu.VMEM((2, tokens, 128), BF),
            pltpu.VMEM((2, tokens, 128), BF),
            pltpu.VMEM((tokens, 256), BF),
            pltpu.SemaphoreType.DMA((4,)),
        ],
        compiler_params=params(40),
        cost_estimate=cost(8e9, 8e6),
        name="attention",
    )(y, xa, xb, *blocks, kx, keep, send)


def proj_weight_kernel(hs, y_ref, w0, w1, w2, w3, out_ref, w_scr, sems):
    for copy in place((w0, w1, w2, w3), w_scr, sems, y_ref[0], 384):
        copy.wait()
    step = 320
    lane = lax.broadcasted_iota(jnp.int32, (step, 128), 1)
    for r in range(0, w_scr.shape[0], step):
        x = w_scr[r : r + step, :].astype(F32)
        for h in range(2):
            turn = 256 - (96 + hs * h)
            p = jnp.where(lane < hs, pltpu.roll(x, turn, 1)[:, :128], 0.0)
            out_ref[r : r + step, 128 * h : 128 * h + 128] = p.astype(BF)


def proj_weights(y, blocks, hs):
    rows = blocks[0].shape[0]
    return pl.pallas_call(
        functools.partial(proj_weight_kernel, hs),
        out_shape=jax.ShapeDtypeStruct((4 * rows, 256), BF),
        in_specs=whole(1, SMEM) + whole(4, pl.ANY),
        out_specs=whole(1)[0],
        scratch_shapes=[pltpu.VMEM((4 * rows, 256), BF), pltpu.SemaphoreType.DMA((4,))],
        compiler_params=params(16),
        cost_estimate=cost(1e9, 3e6),
        name="proj_weights",
    )(y, *blocks)


def projection_kernel(kept, other, w_kept, w_other, base, mine, *sent):
    part = dot_t(kept[...], w_kept[...]) + dot_t(other[...], w_other[...])
    mine[...] = base[...] + part[:128]
    for k, out in enumerate(sent):
        out[...] = part[128 * (k + 1) : 128 * (k + 2)].astype(BF)


def projection(kept, other, w_kept, w_other, base):
    return pl.pallas_call(
        projection_kernel,
        out_shape=[jax.ShapeDtypeStruct(base.shape, F32)] + [jax.ShapeDtypeStruct(base.shape, BF)] * 3,
        in_specs=whole(5),
        out_specs=whole(4),
        compiler_params=params(16),
        cost_estimate=cost(1e9, 4e6),
        name="projection",
    )(kept, other, w_kept, w_other, base)


def merged_kernel(gain, mine, a, b, d, merged_ref, out_ref):
    merged = mine[...] + a[...].astype(F32) + b[...].astype(F32) + d[...].astype(F32)
    merged_ref[...] = merged
    out_ref[...] = layer_norm(merged, gain[...]).astype(BF)


def merged_norm(gain, mine, received):
    return pl.pallas_call(
        merged_kernel,
        out_shape=[jax.ShapeDtypeStruct(mine.shape, F32), jax.ShapeDtypeStruct(mine.shape, BF)],
        in_specs=whole(5),
        out_specs=whole(2),
        compiler_params=params(16),
        cost_estimate=cost(1e8, 2e6),
        name="merged_norm",
    )(gain, mine, *received)


def mlp_weights_kernel(yz_ref, *refs):
    *blocks, up, down = refs
    half = up.shape[2]
    zs = len(blocks)
    y, z = yz_ref[0], yz_ref[1]
    ys = blocks[0].shape[0]
    for k, block in enumerate(blocks):
        for j in range(ys):
            at = lax.rem(y + j, ys) * zs + lax.rem(z + k, zs)
            up[at] = block[j, :, :half]
            down[at] = block[j, :, half:]


def mlp_weights(yz, blocks):
    ys, rows, cols = blocks[0].shape
    total = ys * len(blocks)
    return pl.pallas_call(
        mlp_weights_kernel,
        out_shape=[jax.ShapeDtypeStruct((total, rows, cols // 2), BF)] * 2,
        in_specs=whole(1, SMEM) + whole(len(blocks)),
        out_specs=whole(2),
        compiler_params=params(16),
        cost_estimate=cost(1e9, 6e6),
        name="mlp_weights",
    )(yz, *blocks)


def mlp_kernel(n, *refs):
    ins, (up_a, up_b, down_a, down_b, bias_a, bias_b) = refs[:n], refs[n : n + 6]
    outs, (rows, hidden) = refs[n + 6 : 2 * n + 6], refs[2 * n + 6 :]
    for k, r in enumerate(ins):
        rows[128 * k : 128 * k + 128, :] = r[...]
    half = up_a.shape[1]
    for i, (up, bias) in enumerate(((up_a, bias_a), (up_b, bias_b))):
        h = jax.nn.gelu(dot(rows[...], up[...]) + bias[...])
        hidden[:, half * i : half * (i + 1)] = h.astype(BF)
    total = dot_t(hidden[:, :half], down_a[...]) + dot_t(hidden[:, half:], down_b[...])
    for k, out in enumerate(outs):
        out[...] = total[128 * k : 128 * k + 128].astype(out.dtype)


def mlp(rows, ups, downs, biases, kind):
    shape = rows[0].shape
    n = len(rows)
    return pl.pallas_call(
        functools.partial(mlp_kernel, n),
        out_shape=[jax.ShapeDtypeStruct(shape, kind)] * n,
        in_specs=whole(n + 6),
        out_specs=whole(n),
        scratch_shapes=[
            pltpu.VMEM((n * shape[0], shape[1]), BF),
            pltpu.VMEM((n * shape[0], 2 * ups[0].shape[1]), BF),
        ],
        compiler_params=params(24),
        cost_estimate=cost(1.5e9 * n, 8e6),
    )(*rows, *ups, *downs, *(b[None] for b in biases))


def turned(table, x, c):
    blocks = table.reshape(4, 2, 128)
    blocks = lax.dynamic_slice_in_dim(jnp.concatenate([blocks, blocks]), x, 4, 0)
    mine = lax.dynamic_index_in_dim(blocks, c, 1, keepdims=False)
    other = lax.dynamic_index_in_dim(blocks, 1 - c, 1, keepdims=False)
    return jnp.concatenate([mine.reshape(-1), other.reshape(-1)])


def tables(sizes, sources, targets, order, x, c, hs):
    kept = order.shape[0] // 8
    positions = jnp.arange(1024, dtype=jnp.int32)
    hits = positions[None, :] == sources[:, None]
    dest = positions + jnp.sum(jnp.where(hits, targets[:, None] - positions[None, :], 0), axis=0)
    dest = turned(dest, x, c)
    size = turned(sizes, x, c)
    order = jnp.pad(order.reshape(8, kept), ((0, 0), (0, 128 - kept)), constant_values=-1)
    order = turned(order.reshape(-1), x, c).reshape(2, 512)
    table = jnp.where(order[:, :, None] == dest, size, 0.0)
    merged_size = jnp.sum(table, axis=-1, keepdims=True)
    table = (table / jnp.where(merged_size == 0.0, 1.0, merged_size)).astype(BF)
    bias = jnp.log(size) * math.sqrt(hs)
    high = lax.reduce_precision(bias, 8, 7)
    mid = lax.reduce_precision(bias - high, 8, 7)
    low = bias - high - mid
    lane = jnp.arange(128)[None, :] - hs
    kx = jnp.where(lane == 0, high[:, None], jnp.where(lane == 1, mid[:, None], jnp.where(lane == 2, low[:, None], 0.0)))
    return table[0], table[1], kx


def shards(tokens, sizes, ln1_gain, qkv_weight, proj_weight, ln2_gain, fc1_weight,
           fc1_bias, fc2_weight, pair_source, pair_target, kept_order):
    y, z, x, c = (lax.axis_index(a) for a in ("y", "z", "x", "c"))
    zs = lax.axis_size("z")
    width = tokens.shape[2]
    hs = width // HEADS
    own = tokens[0]
    kept = kept_order.shape[1] // 8
    at_y = y[None]

    near = [own] + [shift(own, "x", -k) for k in (1, 2, 3)]
    raw_mine, normed_mine = norms(ln1_gain[None], near)
    raw_other = shift(raw_mine, "c", 1)
    normed_other = norm_other(ln1_gain[None], raw_other)

    qkvp = jnp.concatenate([qkv_weight[0], qkv_weight[1], qkv_weight[2], proj_weight.T], axis=1)
    by_z = lax.all_to_all(jnp.broadcast_to(qkvp, (zs, *qkvp.shape)), "z", 0, 0, tiled=True)
    by_z = by_z.reshape(-1, qkvp.shape[1])
    by_y = [by_z] + [shift(by_z, "y", -j) for j in (1, 2, 3)]

    updown = jnp.concatenate([fc1_weight, fc2_weight.T], axis=1)
    stack = jnp.stack([updown] + [shift(updown, "y", -j) for j in (1, 2, 3)])
    ring = {0: stack}
    for k in range(1, 4):
        ring[k] = shift(ring[k - 1], "z", -1)
        ring[zs - k] = shift(ring[(zs - k + 1) % zs], "z", 1)
    ring[4] = jnp.concatenate([shift(ring[3][:2], "z", -1), shift(ring[5][2:], "z", 1)])
    up, down = mlp_weights(jnp.stack([y, z]), [ring[k] for k in range(zs)])
    up = up.reshape(width, -1)
    down = down.reshape(width, -1)
    ups = (up, shift(up, "c", 1))
    downs = (down, shift(down, "c", 1))
    biases = (fc1_bias, shift(fc1_bias, "c", 1))

    keep, send, kx = tables(sizes[0], pair_source[0], pair_target[0], kept_order[0], x, c, hs)
    base = dot(keep[:128, :512], raw_mine) + dot(keep[:128, 512:], raw_other)

    proj = proj_weights(at_y, by_y, hs)
    proj_other = shift(proj, "c", 1)
    kept_rows, sent_rows = attention(at_y, normed_mine, normed_other, by_y, kx, keep, send, hs)
    other_rows = shift(sent_rows, "c", 1)

    mine, *sent = projection(kept_rows, other_rows, proj, proj_other, base)
    received = [shift(sent[k], "x", k + 1) for k in range(3)]
    merged, normed2 = merged_norm(ln2_gain[None], mine, received)
    rows = [shift(normed2, "x", -k) for k in (1, 2, 3)]
    (mine,) = mlp([normed2], ups, downs, biases, F32)
    first, third = mlp([rows[0], rows[2]], ups, downs, biases, BF)
    (second,) = mlp([rows[1]], ups, downs, biases, BF)
    received = [shift(b, "x", k).astype(F32) for k, b in ((1, first), (3, third), (2, second))]
    out = merged + mine + received[0] + received[1] + received[2]
    return out[:kept].astype(BF)[None]


def solution(mesh):
    fine = Mesh(mesh.devices.reshape(4, 8, 4, 2), ("y", "z", "x", "c"))
    dp, mp = ("y", "z"), ("x", "c")
    return jax.shard_map(
        shards,
        mesh=fine,
        in_specs=(
            P(dp, mp, None),
            P(dp, None),
            P(),
            P(None, dp, mp),
            P(mp, dp),
            P(),
            P(dp, mp),
            P(mp),
            P(mp, dp),
            P(dp, None),
            P(dp, None),
            P(dp, None),
        ),
        out_specs=P(dp, mp, None),
        check_vma=False,
    )
```

```python
import functools
import math

import jax
import jax.numpy as jnp
from jax import lax
from jax.experimental import pallas as pl
from jax.experimental.pallas import tpu as pltpu
from jax.sharding import Mesh, PartitionSpec as P

HEADS = 16
BF = jnp.bfloat16
F32 = jnp.float32
VMEM = pltpu.VMEM
SMEM = pltpu.SMEM


def shift(x, axis, by):
    n = lax.axis_size(axis)
    return lax.ppermute(x, axis, [(i, (i + by) % n) for i in range(n)])


def layer_norm(values, gain):
    center = values - jnp.mean(values, axis=-1, keepdims=True)
    spread = jnp.mean(center * center, axis=-1, keepdims=True)
    return center * lax.rsqrt(spread + 1e-06) * gain


def dot_t(a, b):
    return lax.dot_general(a, b, (((1,), (1,)), ((), ())), preferred_element_type=F32)


def dot(a, b):
    return jnp.dot(a, b, preferred_element_type=F32)


def whole(n, space=VMEM):
    return [pl.BlockSpec(memory_space=space)] * n


def params(mib):
    return pltpu.CompilerParams(vmem_limit_bytes=mib * 2**20)


def cost(flops, nbytes):
    return pl.CostEstimate(flops=int(flops), bytes_accessed=int(nbytes), transcendentals=0)


def norm_kernel(gain_ref, *refs):
    blocks, (raw_ref, out_ref) = refs[:-2], refs[-2:]
    step = 64
    for n, block in enumerate(blocks):
        rows = block.shape[0]

        @pl.loop(0, rows // step)
        def _(i):
            at = pl.multiple_of(i * step, step)
            x = block[pl.ds(at, step), :]
            raw_ref[pl.ds(n * rows + at, step), :] = x
            out_ref[pl.ds(n * rows + at, step), :] = layer_norm(x.astype(F32), gain_ref[...]).astype(BF)


def norm_other_kernel(gain_ref, block, out_ref):
    step = 64

    @pl.loop(0, block.shape[0] // step)
    def _(i):
        at = pl.ds(pl.multiple_of(i * step, step), step)
        out_ref[at, :] = layer_norm(block[at, :].astype(F32), gain_ref[...]).astype(BF)


def norms(gain, blocks):
    rows = sum(b.shape[0] for b in blocks)
    shape = jax.ShapeDtypeStruct((rows, blocks[0].shape[1]), BF)
    return pl.pallas_call(
        norm_kernel,
        out_shape=[shape, shape],
        in_specs=whole(1 + len(blocks)),
        out_specs=whole(2),
        compiler_params=params(16),
        cost_estimate=cost(2e9, 4e6),
        name="norm_mine",
    )(gain, *blocks)


def norm_other(gain, block):
    return pl.pallas_call(
        norm_other_kernel,
        out_shape=jax.ShapeDtypeStruct(block.shape, BF),
        in_specs=whole(2),
        out_specs=whole(1)[0],
        compiler_params=params(16),
        cost_estimate=cost(2e9, 3e6),
        name="norm_other",
    )(gain, block)


def place(blocks, scratch, sems, first, left=0):
    rows = blocks[0].shape[0]
    right = left + scratch.shape[1]
    copies = []
    for j, block in enumerate(blocks):
        start = pl.multiple_of(lax.rem(first + j, len(blocks)) * rows, 64)
        copies.append(pltpu.make_async_copy(block.at[:, left:right], scratch.at[pl.ds(start, rows), :], sems.at[j]))
    for copy in copies:
        copy.start()
    return copies


def attention_kernel(hs, y_ref, xa_ref, xb_ref, w0, w1, w2, w3, kx_ref, keep_ref, send_ref,
                     out_keep, out_send, w_scr, qkv_scr, q_scr, k_scr, v_scr, att_scr, sems):
    half = xa_ref.shape[0]
    tokens = 2 * half
    for copy in place((w0, w1, w2, w3), w_scr, sems, y_ref[0]):
        copy.wait()
    chunk = 256
    qkv_scr[:half, :] = dot(xa_ref[...], w_scr[...])
    qkv_scr[half:, :] = dot(xb_ref[...], w_scr[...])
    scale = math.log2(math.e) / math.sqrt(hs)

    def piece(j):
        first, offset = divmod(hs * j, 128)
        width = 128 if offset + hs <= 128 else 256
        x = qkv_scr[:, 128 * first : 128 * first + width]
        if offset:
            x = pltpu.roll(x, width - offset, 1)
        return x[:, :128]

    lane = lax.broadcasted_iota(jnp.int32, (tokens, 128), 1)
    real = lane < hs
    for h in range(2):
        ones = jnp.where(lane < hs + 3, 1.0, 0.0)
        q_scr[h] = jnp.where(real, piece(h), ones).astype(BF)
        k_scr[h] = jnp.where(real, piece(2 + h), kx_ref[...]).astype(BF)
        v_scr[h] = jnp.where(real, piece(4 + h), ones).astype(BF)

    @pl.loop(0, 2)
    def _(h):
        for r in range(0, tokens, chunk):
            s = dot_t(q_scr[h, r : r + chunk, :], k_scr[h])
            top = jnp.max(s, axis=-1, keepdims=True)
            p = jnp.exp2((s - top) * scale).astype(BF)
            o = dot(p, v_scr[h])
            o = o / o[:, hs : hs + 1]
            o = jnp.where(lane[:chunk] < hs, o, 0.0)
            att_scr[r : r + chunk, pl.ds(pl.multiple_of(128 * h, 128), 128)] = o.astype(BF)

    out_send[...] = dot(send_ref[...], att_scr[...]).astype(BF)
    out_keep[...] = dot(keep_ref[...], att_scr[...]).astype(BF)


def attention(y, xa, xb, blocks, kx, keep, send, hs):
    tokens = 2 * xa.shape[0]
    rows = keep.shape[0]
    return pl.pallas_call(
        functools.partial(attention_kernel, hs),
        out_shape=[jax.ShapeDtypeStruct((rows, 256), BF)] * 2,
        in_specs=whole(1, SMEM) + whole(2) + whole(4, pl.ANY) + whole(3),
        out_specs=whole(2),
        scratch_shapes=[
            pltpu.VMEM((4 * blocks[0].shape[0], 512), BF),
            pltpu.VMEM((tokens, 512), F32),
            pltpu.VMEM((2, tokens, 128), BF),
            pltpu.VMEM((2, tokens, 128), BF),
            pltpu.VMEM((2, tokens, 128), BF),
            pltpu.VMEM((tokens, 256), BF),
            pltpu.SemaphoreType.DMA((4,)),
        ],
        compiler_params=params(40),
        cost_estimate=cost(8e9, 8e6),
        name="attention",
    )(y, xa, xb, *blocks, kx, keep, send)


def proj_weight_kernel(hs, y_ref, w0, w1, w2, w3, out_ref, w_scr, sems):
    for copy in place((w0, w1, w2, w3), w_scr, sems, y_ref[0], 384):
        copy.wait()
    step = 320
    lane = lax.broadcasted_iota(jnp.int32, (step, 128), 1)

    @pl.loop(0, w_scr.shape[0] // step)
    def _(i):
        at = pl.ds(pl.multiple_of(i * step, step), step)
        x = w_scr[at, :].astype(F32)
        for h in range(2):
            turn = 256 - (96 + hs * h)
            p = jnp.where(lane < hs, pltpu.roll(x, turn, 1)[:, :128], 0.0)
            out_ref[at, 128 * h : 128 * h + 128] = p.astype(BF)


def proj_weights(y, blocks, hs):
    rows = blocks[0].shape[0]
    return pl.pallas_call(
        functools.partial(proj_weight_kernel, hs),
        out_shape=jax.ShapeDtypeStruct((4 * rows, 256), BF),
        in_specs=whole(1, SMEM) + whole(4, pl.ANY),
        out_specs=whole(1)[0],
        scratch_shapes=[pltpu.VMEM((4 * rows, 256), BF), pltpu.SemaphoreType.DMA((4,))],
        compiler_params=params(16),
        cost_estimate=cost(1e9, 3e6),
        name="proj_weights",
    )(y, *blocks)


def projection_kernel(kept, other, w_kept, w_other, base, mine, *sent):
    part = dot_t(kept[...], w_kept[...]) + dot_t(other[...], w_other[...])
    mine[...] = base[...] + part[:128]
    for k, out in enumerate(sent):
        out[...] = part[128 * (k + 1) : 128 * (k + 2)].astype(BF)


def projection(kept, other, w_kept, w_other, base):
    return pl.pallas_call(
        projection_kernel,
        out_shape=[jax.ShapeDtypeStruct(base.shape, F32)] + [jax.ShapeDtypeStruct(base.shape, BF)] * 3,
        in_specs=whole(5),
        out_specs=whole(4),
        compiler_params=params(16),
        cost_estimate=cost(1e9, 4e6),
        name="projection",
    )(kept, other, w_kept, w_other, base)


def merged_kernel(gain, mine, a, b, d, merged_ref, out_ref):
    merged = mine[...] + a[...].astype(F32) + b[...].astype(F32) + d[...].astype(F32)
    merged_ref[...] = merged
    out_ref[...] = layer_norm(merged, gain[...]).astype(BF)


def merged_norm(gain, mine, received):
    return pl.pallas_call(
        merged_kernel,
        out_shape=[jax.ShapeDtypeStruct(mine.shape, F32), jax.ShapeDtypeStruct(mine.shape, BF)],
        in_specs=whole(5),
        out_specs=whole(2),
        compiler_params=params(16),
        cost_estimate=cost(1e8, 2e6),
        name="merged_norm",
    )(gain, mine, *received)


def mlp_weights_kernel(yz_ref, *refs):
    *blocks, up, down = refs
    half = up.shape[2]
    zs = len(blocks)
    y, z = yz_ref[0], yz_ref[1]
    ys = blocks[0].shape[0]
    for k, block in enumerate(blocks):
        for j in range(ys):
            at = lax.rem(y + j, ys) * zs + lax.rem(z + k, zs)
            up[at] = block[j, :, :half]
            down[at] = block[j, :, half:]


def mlp_weights(yz, blocks):
    ys, rows, cols = blocks[0].shape
    total = ys * len(blocks)
    return pl.pallas_call(
        mlp_weights_kernel,
        out_shape=[jax.ShapeDtypeStruct((total, rows, cols // 2), BF)] * 2,
        in_specs=whole(1, SMEM) + whole(len(blocks)),
        out_specs=whole(2),
        compiler_params=params(16),
        cost_estimate=cost(1e9, 6e6),
        name="mlp_weights",
    )(yz, *blocks)


def mlp_kernel(n, *refs):
    ins, (up_a, up_b, down_a, down_b, bias_a, bias_b) = refs[:n], refs[n : n + 6]
    outs, (rows, hidden) = refs[n + 6 : 2 * n + 6], refs[2 * n + 6 :]
    for k, r in enumerate(ins):
        rows[128 * k : 128 * k + 128, :] = r[...]
    half = up_a.shape[1]
    for i, (up, bias) in enumerate(((up_a, bias_a), (up_b, bias_b))):
        h = jax.nn.gelu(dot(rows[...], up[...]) + bias[...])
        hidden[:, half * i : half * (i + 1)] = h.astype(BF)
    total = dot_t(hidden[:, :half], down_a[...]) + dot_t(hidden[:, half:], down_b[...])
    for k, out in enumerate(outs):
        out[...] = total[128 * k : 128 * k + 128].astype(out.dtype)


def mlp(rows, ups, downs, biases, kind):
    shape = rows[0].shape
    n = len(rows)
    return pl.pallas_call(
        functools.partial(mlp_kernel, n),
        out_shape=[jax.ShapeDtypeStruct(shape, kind)] * n,
        in_specs=whole(n + 6),
        out_specs=whole(n),
        scratch_shapes=[
            pltpu.VMEM((n * shape[0], shape[1]), BF),
            pltpu.VMEM((n * shape[0], 2 * ups[0].shape[1]), BF),
        ],
        compiler_params=params(24),
        cost_estimate=cost(1.5e9 * n, 8e6),
    )(*rows, *ups, *downs, *(b[None] for b in biases))


def turned(table, x, c):
    blocks = table.reshape(4, 2, 128)
    blocks = lax.dynamic_slice_in_dim(jnp.concatenate([blocks, blocks]), x, 4, 0)
    mine = lax.dynamic_index_in_dim(blocks, c, 1, keepdims=False)
    other = lax.dynamic_index_in_dim(blocks, 1 - c, 1, keepdims=False)
    return jnp.concatenate([mine.reshape(-1), other.reshape(-1)])


def tables(sizes, sources, targets, order, x, c, hs):
    kept = order.shape[0] // 8
    positions = jnp.arange(1024, dtype=jnp.int32)
    hits = positions[None, :] == sources[:, None]
    dest = positions + jnp.sum(jnp.where(hits, targets[:, None] - positions[None, :], 0), axis=0)
    dest = turned(dest, x, c)
    size = turned(sizes, x, c)
    order = jnp.pad(order.reshape(8, kept), ((0, 0), (0, 128 - kept)), constant_values=-1)
    order = turned(order.reshape(-1), x, c).reshape(2, 512)
    table = jnp.where(order[:, :, None] == dest, size, 0.0)
    merged_size = jnp.sum(table, axis=-1, keepdims=True)
    table = (table / jnp.where(merged_size == 0.0, 1.0, merged_size)).astype(BF)
    bias = jnp.log(size) * math.sqrt(hs)
    high = lax.reduce_precision(bias, 8, 7)
    mid = lax.reduce_precision(bias - high, 8, 7)
    low = bias - high - mid
    lane = jnp.arange(128)[None, :] - hs
    kx = jnp.where(lane == 0, high[:, None], jnp.where(lane == 1, mid[:, None], jnp.where(lane == 2, low[:, None], 0.0)))
    return table[0], table[1], kx


def shards(tokens, sizes, ln1_gain, qkv_weight, proj_weight, ln2_gain, fc1_weight,
           fc1_bias, fc2_weight, pair_source, pair_target, kept_order):
    y, z, x, c = (lax.axis_index(a) for a in ("y", "z", "x", "c"))
    zs = lax.axis_size("z")
    width = tokens.shape[2]
    hs = width // HEADS
    own = tokens[0]
    kept = kept_order.shape[1] // 8
    at_y = y[None]

    near = [own] + [shift(own, "x", -k) for k in (1, 2, 3)]
    raw_mine, normed_mine = norms(ln1_gain[None], near)
    raw_other = shift(raw_mine, "c", 1)
    normed_other = norm_other(ln1_gain[None], raw_other)

    qkvp = jnp.concatenate([qkv_weight[0], qkv_weight[1], qkv_weight[2], proj_weight.T], axis=1)
    by_z = lax.all_to_all(jnp.broadcast_to(qkvp, (zs, *qkvp.shape)), "z", 0, 0, tiled=True)
    by_z = by_z.reshape(-1, qkvp.shape[1])
    by_y = [by_z] + [shift(by_z, "y", -j) for j in (1, 2, 3)]

    updown = jnp.concatenate([fc1_weight, fc2_weight.T], axis=1)
    stack = jnp.stack([updown] + [shift(updown, "y", -j) for j in (1, 2, 3)])
    ring = {0: stack}
    for k in range(1, 4):
        ring[k] = shift(ring[k - 1], "z", -1)
        ring[zs - k] = shift(ring[(zs - k + 1) % zs], "z", 1)
    ring[zs // 2] = shift(ring[zs // 2 - 1], "z", -1)
    up, down = mlp_weights(jnp.stack([y, z]), [ring[k] for k in range(zs)])
    up = up.reshape(width, -1)
    down = down.reshape(width, -1)
    ups = (up, shift(up, "c", 1))
    downs = (down, shift(down, "c", 1))
    biases = (fc1_bias, shift(fc1_bias, "c", 1))

    keep, send, kx = tables(sizes[0], pair_source[0], pair_target[0], kept_order[0], x, c, hs)
    base = dot(keep[:128, :512], raw_mine) + dot(keep[:128, 512:], raw_other)

    proj = proj_weights(at_y, by_y, hs)
    proj_other = shift(proj, "c", 1)
    kept_rows, sent_rows = attention(at_y, normed_mine, normed_other, by_y, kx, keep, send, hs)
    other_rows = shift(sent_rows, "c", 1)

    mine, *sent = projection(kept_rows, other_rows, proj, proj_other, base)
    received = [shift(sent[k], "x", k + 1) for k in range(3)]
    merged, normed2 = merged_norm(ln2_gain[None], mine, received)
    rows = [shift(normed2, "x", -k) for k in (1, 2, 3)]
    (mine,) = mlp([normed2], ups, downs, biases, F32)
    first, third = mlp([rows[0], rows[2]], ups, downs, biases, BF)
    (second,) = mlp([rows[1]], ups, downs, biases, BF)
    received = [shift(b, "x", k).astype(F32) for k, b in ((1, first), (3, third), (2, second))]
    out = merged + mine + received[0] + received[1] + received[2]
    return out[:kept].astype(BF)[None]


def solution(mesh):
    fine = Mesh(mesh.devices.reshape(4, 8, 4, 2), ("y", "z", "x", "c"))
    dp, mp = ("y", "z"), ("x", "c")
    return jax.shard_map(
        shards,
        mesh=fine,
        in_specs=(
            P(dp, mp, None),
            P(dp, None),
            P(),
            P(None, dp, mp),
            P(mp, dp),
            P(),
            P(dp, mp),
            P(mp),
            P(mp, dp),
            P(dp, None),
            P(dp, None),
            P(dp, None),
        ),
        out_specs=P(dp, mp, None),
        check_vma=False,
    )
```

```python
import functools
import math

import jax
import jax.numpy as jnp
from jax import lax
from jax.experimental import pallas as pl
from jax.experimental.pallas import tpu as pltpu
from jax.sharding import Mesh, PartitionSpec as P

HEADS = 16
BF = jnp.bfloat16
F32 = jnp.float32
VMEM = pltpu.VMEM
SMEM = pltpu.SMEM


def shift(x, axis, by):
    n = lax.axis_size(axis)
    return lax.ppermute(x, axis, [(i, (i + by) % n) for i in range(n)])


def layer_norm(values, gain):
    center = values - jnp.mean(values, axis=-1, keepdims=True)
    spread = jnp.mean(center * center, axis=-1, keepdims=True)
    return center * lax.rsqrt(spread + 1e-06) * gain


def dot_t(a, b):
    return lax.dot_general(a, b, (((1,), (1,)), ((), ())), preferred_element_type=F32)


def dot(a, b):
    return jnp.dot(a, b, preferred_element_type=F32)


def whole(n, space=VMEM):
    return [pl.BlockSpec(memory_space=space)] * n


def params(mib):
    return pltpu.CompilerParams(vmem_limit_bytes=mib * 2**20)


def cost(flops, nbytes):
    return pl.CostEstimate(flops=int(flops), bytes_accessed=int(nbytes), transcendentals=0)


def norm_kernel(gain_ref, *refs):
    blocks, (raw_ref, out_ref) = refs[:-2], refs[-2:]
    step = 64
    for n, block in enumerate(blocks):
        rows = block.shape[0]

        @pl.loop(0, rows // step)
        def _(i):
            at = pl.multiple_of(i * step, step)
            x = block[pl.ds(at, step), :]
            raw_ref[pl.ds(n * rows + at, step), :] = x
            out_ref[pl.ds(n * rows + at, step), :] = layer_norm(x.astype(F32), gain_ref[...]).astype(BF)


def norm_other_kernel(gain_ref, block, out_ref):
    step = 64

    @pl.loop(0, block.shape[0] // step)
    def _(i):
        at = pl.ds(pl.multiple_of(i * step, step), step)
        out_ref[at, :] = layer_norm(block[at, :].astype(F32), gain_ref[...]).astype(BF)


def norms(gain, blocks):
    rows = sum(b.shape[0] for b in blocks)
    shape = jax.ShapeDtypeStruct((rows, blocks[0].shape[1]), BF)
    return pl.pallas_call(
        norm_kernel,
        out_shape=[shape, shape],
        in_specs=whole(1 + len(blocks)),
        out_specs=whole(2),
        compiler_params=params(16),
        cost_estimate=cost(2e9, 4e6),
        name="norm_mine",
    )(gain, *blocks)


def norm_other(gain, block):
    return pl.pallas_call(
        norm_other_kernel,
        out_shape=jax.ShapeDtypeStruct(block.shape, BF),
        in_specs=whole(2),
        out_specs=whole(1)[0],
        compiler_params=params(16),
        cost_estimate=cost(2e9, 3e6),
        name="norm_other",
    )(gain, block)


def place(blocks, scratch, sems, first, left=0):
    rows = blocks[0].shape[0]
    right = left + scratch.shape[1]
    copies = []
    for j, block in enumerate(blocks):
        start = pl.multiple_of(lax.rem(first + j, len(blocks)) * rows, 64)
        copies.append(pltpu.make_async_copy(block.at[:, left:right], scratch.at[pl.ds(start, rows), :], sems.at[j]))
    for copy in copies:
        copy.start()
    return copies


def attention_kernel(hs, y_ref, xa_ref, xb_ref, w0, w1, w2, w3, kx_ref, keep_ref, send_ref,
                     out_keep, out_send, w_scr, qkv_scr, q_scr, k_scr, v_scr, att_scr, sems):
    half = xa_ref.shape[0]
    tokens = 2 * half
    for copy in place((w0, w1, w2, w3), w_scr, sems, y_ref[0]):
        copy.wait()
    chunk = 256
    qkv_scr[:half, :] = dot(xa_ref[...], w_scr[...])
    qkv_scr[half:, :] = dot(xb_ref[...], w_scr[...])
    scale = math.log2(math.e) / math.sqrt(hs)

    def piece(j):
        first, offset = divmod(hs * j, 128)
        width = 128 if offset + hs <= 128 else 256
        x = qkv_scr[:, 128 * first : 128 * first + width]
        if offset:
            x = pltpu.roll(x, width - offset, 1)
        return x[:, :128]

    lane = lax.broadcasted_iota(jnp.int32, (tokens, 128), 1)
    real = lane < hs
    for h in range(2):
        ones = jnp.where(lane < hs + 3, 1.0, 0.0)
        q_scr[h] = jnp.where(real, piece(h), ones).astype(BF)
        k_scr[h] = jnp.where(real, piece(2 + h), kx_ref[...]).astype(BF)
        v_scr[h] = jnp.where(real, piece(4 + h), ones).astype(BF)

    @pl.loop(0, 2)
    def _(h):
        for r in range(0, tokens, chunk):
            s = dot_t(q_scr[h, r : r + chunk, :], k_scr[h])
            top = jnp.max(s, axis=-1, keepdims=True)
            p = jnp.exp2((s - top) * scale).astype(BF)
            o = dot(p, v_scr[h])
            o = o / o[:, hs : hs + 1]
            o = jnp.where(lane[:chunk] < hs, o, 0.0)
            att_scr[r : r + chunk, pl.ds(pl.multiple_of(128 * h, 128), 128)] = o.astype(BF)

    out_send[...] = dot(send_ref[...], att_scr[...]).astype(BF)
    out_keep[...] = dot(keep_ref[...], att_scr[...]).astype(BF)


def attention(y, xa, xb, blocks, kx, keep, send, hs):
    tokens = 2 * xa.shape[0]
    rows = keep.shape[0]
    return pl.pallas_call(
        functools.partial(attention_kernel, hs),
        out_shape=[jax.ShapeDtypeStruct((rows, 256), BF)] * 2,
        in_specs=whole(1, SMEM) + whole(2) + whole(4, pl.ANY) + whole(3),
        out_specs=whole(2),
        scratch_shapes=[
            pltpu.VMEM((4 * blocks[0].shape[0], 512), BF),
            pltpu.VMEM((tokens, 512), F32),
            pltpu.VMEM((2, tokens, 128), BF),
            pltpu.VMEM((2, tokens, 128), BF),
            pltpu.VMEM((2, tokens, 128), BF),
            pltpu.VMEM((tokens, 256), BF),
            pltpu.SemaphoreType.DMA((4,)),
        ],
        compiler_params=params(40),
        cost_estimate=cost(8e9, 8e6),
        name="attention",
    )(y, xa, xb, *blocks, kx, keep, send)


def proj_weight_kernel(hs, y_ref, w0, w1, w2, w3, out_ref, w_scr, sems):
    for copy in place((w0, w1, w2, w3), w_scr, sems, y_ref[0], 384):
        copy.wait()
    step = 320
    lane = lax.broadcasted_iota(jnp.int32, (step, 128), 1)

    @pl.loop(0, w_scr.shape[0] // step)
    def _(i):
        at = pl.ds(pl.multiple_of(i * step, step), step)
        x = w_scr[at, :].astype(F32)
        for h in range(2):
            turn = 256 - (96 + hs * h)
            p = jnp.where(lane < hs, pltpu.roll(x, turn, 1)[:, :128], 0.0)
            out_ref[at, 128 * h : 128 * h + 128] = p.astype(BF)


def proj_weights(y, blocks, hs):
    rows = blocks[0].shape[0]
    return pl.pallas_call(
        functools.partial(proj_weight_kernel, hs),
        out_shape=jax.ShapeDtypeStruct((4 * rows, 256), BF),
        in_specs=whole(1, SMEM) + whole(4, pl.ANY),
        out_specs=whole(1)[0],
        scratch_shapes=[pltpu.VMEM((4 * rows, 256), BF), pltpu.SemaphoreType.DMA((4,))],
        compiler_params=params(16),
        cost_estimate=cost(1e9, 3e6),
        name="proj_weights",
    )(y, *blocks)


def projection_kernel(kept, other, w_kept, w_other, base, mine, *sent):
    part = dot_t(kept[...], w_kept[...]) + dot_t(other[...], w_other[...])
    mine[...] = base[...] + part[:128]
    for k, out in enumerate(sent):
        out[...] = part[128 * (k + 1) : 128 * (k + 2)].astype(BF)


def projection(kept, other, w_kept, w_other, base):
    return pl.pallas_call(
        projection_kernel,
        out_shape=[jax.ShapeDtypeStruct(base.shape, F32)] + [jax.ShapeDtypeStruct(base.shape, BF)] * 3,
        in_specs=whole(5),
        out_specs=whole(4),
        compiler_params=params(16),
        cost_estimate=cost(1e9, 4e6),
        name="projection",
    )(kept, other, w_kept, w_other, base)


def merged_kernel(gain, mine, a, b, d, merged_ref, out_ref):
    merged = mine[...] + a[...].astype(F32) + b[...].astype(F32) + d[...].astype(F32)
    merged_ref[...] = merged
    out_ref[...] = layer_norm(merged, gain[...]).astype(BF)


def merged_norm(gain, mine, received):
    return pl.pallas_call(
        merged_kernel,
        out_shape=[jax.ShapeDtypeStruct(mine.shape, F32), jax.ShapeDtypeStruct(mine.shape, BF)],
        in_specs=whole(5),
        out_specs=whole(2),
        compiler_params=params(16),
        cost_estimate=cost(1e8, 2e6),
        name="merged_norm",
    )(gain, mine, *received)


def mlp_weights_kernel(yz_ref, *refs):
    *blocks, up, down = refs
    half = up.shape[2]
    zs = len(blocks)
    y, z = yz_ref[0], yz_ref[1]
    ys = blocks[0].shape[0]
    for k, block in enumerate(blocks):
        for j in range(ys):
            at = lax.rem(y + j, ys) * zs + lax.rem(z + k, zs)
            up[at] = block[j, :, :half]
            down[at] = block[j, :, half:]


def mlp_weights(yz, blocks):
    ys, rows, cols = blocks[0].shape
    total = ys * len(blocks)
    return pl.pallas_call(
        mlp_weights_kernel,
        out_shape=[jax.ShapeDtypeStruct((total, rows, cols // 2), BF)] * 2,
        in_specs=whole(1, SMEM) + whole(len(blocks)),
        out_specs=whole(2),
        compiler_params=params(16),
        cost_estimate=cost(1e9, 6e6),
        name="mlp_weights",
    )(yz, *blocks)


def mlp_kernel(n, *refs):
    ins, (up_a, up_b, down_a, down_b, bias_a, bias_b) = refs[:n], refs[n : n + 6]
    *outs, rows, hidden = refs[n + 6 :]
    size = ins[0].shape[0]
    for k, r in enumerate(ins):
        rows[size * k : size * (k + 1), :] = r[...]
    half = up_a.shape[1]
    for i, (up, bias) in enumerate(((up_a, bias_a), (up_b, bias_b))):
        h = jax.nn.gelu(dot(rows[...], up[...]) + bias[...])
        hidden[:, half * i : half * (i + 1)] = h.astype(BF)
    total = dot_t(hidden[:, :half], down_a[...]) + dot_t(hidden[:, half:], down_b[...])
    for k, out in enumerate(outs):
        out[...] = total[128 * k : 128 * k + 128].astype(out.dtype)


def mlp(rows, ups, downs, biases, kind):
    total, width = sum(r.shape[0] for r in rows), rows[0].shape[1]
    n = len(rows)
    blocks = total // 128
    return pl.pallas_call(
        functools.partial(mlp_kernel, n),
        out_shape=[jax.ShapeDtypeStruct((128, width), kind)] * blocks,
        in_specs=whole(n + 6),
        out_specs=whole(blocks),
        scratch_shapes=[
            pltpu.VMEM((total, width), BF),
            pltpu.VMEM((total, 2 * ups[0].shape[1]), BF),
        ],
        compiler_params=params(24),
        cost_estimate=cost(1.5e9 * blocks, 8e6),
    )(*rows, *ups, *downs, *(b[None] for b in biases))


def turned(table, x, c):
    blocks = table.reshape(4, 2, 128)
    blocks = lax.dynamic_slice_in_dim(jnp.concatenate([blocks, blocks]), x, 4, 0)
    mine = lax.dynamic_index_in_dim(blocks, c, 1, keepdims=False)
    other = lax.dynamic_index_in_dim(blocks, 1 - c, 1, keepdims=False)
    return jnp.concatenate([mine.reshape(-1), other.reshape(-1)])


def tables(sizes, sources, targets, order, x, c, hs):
    kept = order.shape[0] // 8
    positions = jnp.arange(1024, dtype=jnp.int32)
    hits = positions[None, :] == sources[:, None]
    dest = positions + jnp.sum(jnp.where(hits, targets[:, None] - positions[None, :], 0), axis=0)
    dest = turned(dest, x, c)
    size = turned(sizes, x, c)
    order = jnp.pad(order.reshape(8, kept), ((0, 0), (0, 128 - kept)), constant_values=-1)
    order = turned(order.reshape(-1), x, c).reshape(2, 512)
    table = jnp.where(order[:, :, None] == dest, size, 0.0)
    merged_size = jnp.sum(table, axis=-1, keepdims=True)
    table = (table / jnp.where(merged_size == 0.0, 1.0, merged_size)).astype(BF)
    bias = jnp.log(size) * math.sqrt(hs)
    high = lax.reduce_precision(bias, 8, 7)
    mid = lax.reduce_precision(bias - high, 8, 7)
    low = bias - high - mid
    lane = jnp.arange(128)[None, :] - hs
    kx = jnp.where(lane == 0, high[:, None], jnp.where(lane == 1, mid[:, None], jnp.where(lane == 2, low[:, None], 0.0)))
    return table[0], table[1], kx


def shards(tokens, sizes, ln1_gain, qkv_weight, proj_weight, ln2_gain, fc1_weight,
           fc1_bias, fc2_weight, pair_source, pair_target, kept_order):
    y, z, x, c = (lax.axis_index(a) for a in ("y", "z", "x", "c"))
    zs = lax.axis_size("z")
    width = tokens.shape[2]
    hs = width // HEADS
    own = tokens[0]
    kept = kept_order.shape[1] // 8
    at_y = y[None]

    near = [own] + [shift(own, "x", -k) for k in (1, 2, 3)]
    raw_mine, normed_mine = norms(ln1_gain[None], near)
    raw_other = shift(raw_mine, "c", 1)
    normed_other = norm_other(ln1_gain[None], raw_other)

    qkvp = jnp.concatenate([qkv_weight[0], qkv_weight[1], qkv_weight[2], proj_weight.T], axis=1)
    by_z = lax.all_to_all(jnp.broadcast_to(qkvp, (zs, *qkvp.shape)), "z", 0, 0, tiled=True)
    by_z = by_z.reshape(-1, qkvp.shape[1])
    by_y = [by_z] + [shift(by_z, "y", -j) for j in (1, 2, 3)]

    updown = jnp.concatenate([fc1_weight, fc2_weight.T], axis=1)
    stack = jnp.stack([updown] + [shift(updown, "y", -j) for j in (1, 2, 3)])
    ring = {0: stack}
    for k in range(1, 4):
        ring[k] = shift(ring[k - 1], "z", -1)
        ring[zs - k] = shift(ring[(zs - k + 1) % zs], "z", 1)
    ring[zs // 2] = shift(ring[zs // 2 - 1], "z", -1)
    up, down = mlp_weights(jnp.stack([y, z]), [ring[k] for k in range(zs)])
    up = up.reshape(width, -1)
    down = down.reshape(width, -1)
    ups = (up, shift(up, "c", 1))
    downs = (down, shift(down, "c", 1))
    biases = (fc1_bias, shift(fc1_bias, "c", 1))

    keep, send, kx = tables(sizes[0], pair_source[0], pair_target[0], kept_order[0], x, c, hs)
    base = dot(keep[:128, :512], raw_mine) + dot(keep[:128, 512:], raw_other)

    proj = proj_weights(at_y, by_y, hs)
    proj_other = shift(proj, "c", 1)
    kept_rows, sent_rows = attention(at_y, normed_mine, normed_other, by_y, kx, keep, send, hs)
    other_rows = shift(sent_rows, "c", 1)

    mine, *sent = projection(kept_rows, other_rows, proj, proj_other, base)
    received = [shift(sent[k], "x", k + 1) for k in range(3)]
    merged, normed2 = merged_norm(ln2_gain[None], mine, received)
    ahead, behind = shift(normed2, "x", -1), shift(normed2, "x", 1)
    far = [shift(ahead[:64], "x", -1), shift(behind[64:], "x", 1)]
    (mine,) = mlp([normed2], ups, downs, biases, F32)
    first, third = mlp([ahead, behind], ups, downs, biases, BF)
    (second,) = mlp(far, ups, downs, biases, BF)
    received = [shift(b, "x", k).astype(F32) for k, b in ((1, first), (3, third), (2, second))]
    out = merged + mine + received[0] + received[1] + received[2]
    return out[:kept].astype(BF)[None]


def solution(mesh):
    fine = Mesh(mesh.devices.reshape(4, 8, 4, 2), ("y", "z", "x", "c"))
    dp, mp = ("y", "z"), ("x", "c")
    return jax.shard_map(
        shards,
        mesh=fine,
        in_specs=(
            P(dp, mp, None),
            P(dp, None),
            P(),
            P(None, dp, mp),
            P(mp, dp),
            P(),
            P(dp, mp),
            P(mp),
            P(mp, dp),
            P(dp, None),
            P(dp, None),
            P(dp, None),
        ),
        out_specs=P(dp, mp, None),
        check_vma=False,
    )
```
